32 devices in a mesh: ctx: 8 (over z, core), head: 4 (over y, x).
Axes of the slice: x: 2, y: 2, z: 4, core: 2. Of those that a mesh axis runs over, the one named last changes fastest.
Arguments:
- queries: bfloat16 [2048, 8192], P(('ctx', 'head')), may hold values from -100 to 100
- keys: bfloat16 [2048, 1024], P(('ctx', 'head')), may hold values from -100 to 100
- values: bfloat16 [2048, 1024], P(('ctx', 'head')), may hold values from -6 to 6
- out_grad: bfloat16 [2048, 8192], P(('ctx', 'head')), may hold values from -6 to 6
- doc_ids: int32 [2048], replicated, may hold values from 0 to 3, never falling along the last dimension, each value on 1 to 1024 neighbouring positions
Outputs:
- query_grad: float32 [2048, 8192], P(('ctx', 'head'))
- key_grad: float32 [2048, 1024], P(('ctx', 'head'))
- value_grad: float32 [2048, 1024], P(('ctx', 'head'))
The draws below stay inside these ranges and needn't reach their ends.
Inputs may be any that keep to these rules, and one draw needn't show every extreme that they name: `doc_ids`: never falling along the sequence; each document holds 1 to 1024 tokens, one exactly 1024.
All inputs are finite; a program needn't handle non-finite values.
Results may differ from the reference program's by a relative error of at most 0.004.
Values may be sent and summed in bfloat16 or wider, within the bound.
A program may use at most 64 MiB of HBM per device.

```python
import math
import jax
import jax.numpy as jnp
import numpy as np
from jax import lax

HEADS = 64
KV_HEADS = 8
HD = 128
BLK = 256
TOKENS = 2048
SPAN = 768
DOCS = 4
MOST_DOC = 1024
N_CTX = 8


def draw_pair(key):
    base = jax.random.fold_in(key, 7)
    key_q, key_k = jax.random.split(base, 2)
    key_vals = jax.random.normal(key_k, (TOKENS, KV_HEADS * HD), jnp.float32)
    query_vals = jax.random.normal(key_q, (TOKENS, HEADS * HD), jnp.float32)
    return (jnp.clip(query_vals, -100.0, 100.0), jnp.clip(key_vals, -100.0, 100.0))


def draw_queries(key, part):
    return draw_pair(key)[0].astype(jnp.bfloat16)


def draw_keys(key, part):
    return draw_pair(key)[1].astype(jnp.bfloat16)


def level_of(stream_key, extent, shards, least, high):
    loudness, own = 1.0, jax.random.fold_in(stream_key, 6)
    for axis_at, shards_of in shards:
        steps = jnp.exp(jax.random.uniform(jax.random.fold_in(own, axis_at), (shards_of,), jnp.float32, least / len(shards), high / len(shards)))
        loudness = loudness * jnp.repeat(steps, extent[axis_at] // shards_of).reshape([-1 if axis == axis_at else 1 for axis in range(len(extent))])
    return loudness


def profile(count, total, limit, slope):
    portions = [(1 << 20) // math.isqrt(rank ** slope) + 1 for rank in range(2, count + 1)]
    spare, given = total - limit - (count - 1), [1] * (count - 1)
    while spare > 0:
        free = [i for i in range(count - 1) if given[i] < limit]
        mass, budget = sum([portions[i] for i in free]), spare
        for i in free:
            more = min(limit - given[i], max(1, budget * portions[i] // mass), spare)
            given[i] = given[i] + more
            spare = spare - more
    return np.array([limit] + given)


def uneven_parts(stream_key, count, total, most, lean):
    if count == 2:
        one = jax.random.randint(stream_key, (), max(1, total - most), min(most, total - 1) + 1)
        return jnp.stack([one, total - one])
    tallies = jnp.asarray(profile(count, total, most, lean), jnp.int32)
    couples = (count - 1) // 2
    donor, sink = tallies[1:1 + 2 * couples:2], tallies[2:2 + 2 * couples:2]
    room = jnp.minimum(donor - 1, most - sink)
    passed = jax.random.randint(jax.random.fold_in(stream_key, 1), (couples,), 0, 1 << 20) % (room + 1)
    tallies = tallies.at[1:1 + 2 * couples:2].set(donor - passed).at[2:2 + 2 * couples:2].set(sink + passed)
    return tallies[jax.random.permutation(jax.random.fold_in(stream_key, 2), count)]


def bell_draw(own_key, extent, width, most, shards=(), kind=jnp.bfloat16):
    factor_of = level_of(own_key, extent, shards, -0.22, 0.18) if shards else 1.0
    entries = jax.random.normal(own_key, extent, jnp.float32) * width * factor_of
    return jnp.minimum(jnp.maximum(entries, -most), most).astype(kind)


def setup_inputs(seed: int = 0) -> dict:
    streams_of = jax.random.split(jax.random.key(seed), 6)
    queries = draw_queries(jax.random.fold_in(streams_of[5], 71), 0)
    keys = draw_keys(jax.random.fold_in(streams_of[5], 71), 0)
    values = bell_draw(streams_of[2], (TOKENS, KV_HEADS * HD), 1.0, 6.0, ((0, 32),))
    out_grad = bell_draw(streams_of[3], (TOKENS, HEADS * HD), 1.0, 6.0, ((0, 32),))
    doc_ids = jnp.searchsorted(jnp.cumsum(uneven_parts(streams_of[4], DOCS, TOKENS, MOST_DOC, 2)), jnp.arange(TOKENS), side="right").astype(jnp.int32)
    return {"queries": queries, "keys": keys, "values": values, "out_grad": out_grad, "doc_ids": doc_ids}


def reference(queries, keys, values, out_grad, doc_ids):
    group_size = HEADS // KV_HEADS
    score_scale = 1.0 / (HD ** 0.5)
    margin = 3 * BLK
    pad_keys = jnp.concatenate([jnp.zeros((margin, KV_HEADS * HD), keys.dtype), keys], 0)
    pad_values = jnp.concatenate([jnp.zeros((margin, KV_HEADS * HD), values.dtype), values], 0)
    pad_docs = jnp.concatenate([jnp.full((margin,), -1, jnp.int32), doc_ids.astype(jnp.int32)], 0)
    zero_acc = jnp.zeros((margin + TOKENS, KV_HEADS, HD), jnp.float32)

    def one_block(carry, block):
        key_acc, value_acc = carry
        first_row = (block * BLK).astype(jnp.int32)
        key_win = lax.dynamic_slice_in_dim(pad_keys, first_row, 4 * BLK, 0).reshape(4 * BLK, KV_HEADS, HD).astype(jnp.float32)
        value_win = lax.dynamic_slice_in_dim(pad_values, first_row, 4 * BLK, 0).reshape(4 * BLK, KV_HEADS, HD).astype(jnp.float32)
        query_blk = lax.dynamic_slice_in_dim(queries, first_row, BLK, 0).reshape(BLK, KV_HEADS, group_size, HD).astype(jnp.float32)
        grad_blk = lax.dynamic_slice_in_dim(out_grad, first_row, BLK, 0).reshape(BLK, KV_HEADS, group_size, HD).astype(jnp.float32)
        query_pos = first_row + jnp.arange(BLK, dtype=jnp.int32)
        key_pos = first_row - margin + jnp.arange(4 * BLK, dtype=jnp.int32)
        query_doc = lax.dynamic_slice_in_dim(doc_ids.astype(jnp.int32), first_row, BLK, 0)
        key_doc = lax.dynamic_slice_in_dim(pad_docs, first_row, 4 * BLK, 0)
        allowed = (key_pos[None, :] <= query_pos[:, None]) & (key_pos[None, :] > query_pos[:, None] - SPAN)
        allowed = allowed & (key_pos[None, :] >= 0) & (query_doc[:, None] == key_doc[None, :])
        scores = jnp.einsum('ikgd,jkd->kgij', query_blk, key_win) * score_scale
        scores = jnp.where(allowed[None, None], scores, -jnp.inf)
        row_max = jnp.max(scores, -1, keepdims=True)
        expo = jnp.exp(scores - row_max)
        weights = expo / jnp.sum(expo, -1, keepdims=True)
        weight_bf = lax.optimization_barrier(weights.astype(jnp.bfloat16)).astype(jnp.float32)
        attended = jnp.einsum('kgij,jkd->ikgd', weight_bf, value_win)
        delta_sum = jnp.transpose(jnp.sum(grad_blk * attended, -1), (1, 2, 0))
        value_part = jnp.einsum('kgij,ikgd->jkd', weight_bf, grad_blk)
        prob_grad = jnp.einsum('ikgd,jkd->kgij', grad_blk, value_win)
        score_grad = lax.optimization_barrier((weights * (prob_grad - delta_sum[..., None])).astype(jnp.bfloat16)).astype(jnp.float32)
        query_full = jnp.einsum('kgij,jkd->ikgd', score_grad, key_win) * score_scale
        key_part = jnp.einsum('kgij,ikgd->jkd', score_grad, query_blk) * score_scale
        zero = jnp.zeros((), jnp.int32)
        key_old = lax.dynamic_slice(key_acc, (first_row, zero, zero), (4 * BLK, KV_HEADS, HD))
        key_acc = lax.dynamic_update_slice(key_acc, key_old + key_part, (first_row, zero, zero))
        value_old = lax.dynamic_slice(value_acc, (first_row, zero, zero), (4 * BLK, KV_HEADS, HD))
        value_acc = lax.dynamic_update_slice(value_acc, value_old + value_part, (first_row, zero, zero))
        return (key_acc, value_acc), query_full.reshape(BLK, HEADS * HD)

    (key_acc, value_acc), query_rows = lax.scan(one_block, (zero_acc, zero_acc), jnp.arange(N_CTX, dtype=jnp.int32))
    query_full = query_rows.reshape(TOKENS, HEADS * HD)
    key_full = key_acc[margin:].reshape(TOKENS, KV_HEADS * HD)
    value_full = value_acc[margin:].reshape(TOKENS, KV_HEADS * HD)
    return (query_full, key_full, value_full)
```

```python
import functools
import math
import jax
import jax.numpy as jnp
from jax import lax
from jax.experimental import pallas as pl
from jax.experimental.pallas import tpu as pltpu
from jax.sharding import PartitionSpec as P

HD = 128
BACK = 3
SLOTS = 4
MESH = pl.DeviceIdType.MESH
NT = (((1,), (1,)), ((), ()))


def flip(v, mask):
    bit = 1
    while bit <= mask:
        if mask & bit:
            v = v + bit * (1 - 2 * ((v // bit) % 2))
        bit *= 2
    return v


def kernel(
    n_ctx, n_head,
    q_ref, k_ref, v_ref, g_ref, doc_ref,
    dq_out, dk_out, dv_out,
    q_buf, g_buf, dq_buf, kv_buf, kt_buf, acc, bias, part_out, part_in, tot_out, tot_in,
    kv_send, kv_recv, in_send, in_recv, up_send, up_recv, last_send, last_recv,
    dq_send, dq_recv, part_send, part_recv, tot_send, tot_recv,
):
    c = lax.axis_index("ctx")
    h = lax.axis_index("head")
    k = c % 2
    z = c // 2
    n_z = n_ctx // 2
    rows = q_ref.shape[0]
    blk = rows * n_head
    jobs, _, n_st, pair, width = q_buf.shape
    heads = width // HD
    scale = 1.0 / HD**0.5
    has_up, has_down, has_two = z + 1 < n_z, z >= 1, z >= 2

    def at(n, size):
        return pl.ds(pl.multiple_of(n * size, size), size)

    def bit_of(v, j):
        return (v // (1 << j % 2)) % 2

    def dev(dk, dh):
        return (flip(c, dk), flip(h, dh))

    mine = [2 * bit_of(h, j) + k for j in range(jobs)]
    plane = [(dk, dh) for dh in range(n_head) for dk in range(2)]
    others = plane[1:]
    up = ((c + 2) % n_ctx, h)
    down = ((c - 2 + n_ctx) % n_ctx, h)

    barrier = pltpu.get_barrier_semaphore()
    for to in [dev(*p) for p in others] + [up, down]:
        pl.semaphore_signal(barrier, inc=1, device_id=to, device_id_type=MESH)
    pl.semaphore_wait(barrier, len(others) + 2)

    def kv_copy(j, t, p):
        dk, dh = p
        slot = 2 * bit_of(flip(h, dh), j) + flip(k, dk)
        src = (k_ref, v_ref)[t].at[:, at(SLOTS * j + slot, HD)]
        dst = kv_buf.at[j, BACK + k, t, at(h, rows)]
        if p == (0, 0):
            return pltpu.make_async_copy(src, dst, kv_recv.at[j, t, 0, 0])
        return pltpu.make_async_remote_copy(
            src_ref=src, dst_ref=dst,
            send_sem=kv_send.at[j, t, dk, dh], recv_sem=kv_recv.at[j, t, dk, dh],
            device_id=dev(dk, dh), device_id_type=MESH,
        )

    def kv_arrived(j, p):
        for t in range(2):
            if p == (0, 0):
                kv_copy(j, t, p).wait()
            else:
                kv_copy(j, t, p).wait_recv()

    def in_copy(j, s, t, dk, db):
        slot = 2 * flip(bit_of(h, j), db) + flip(k, dk)
        src = (q_ref, g_ref)[t].at[:, at((SLOTS * j + slot) * n_st + s, width)]
        dst = (q_buf, g_buf)[t].at[j, k, s, at(bit_of(h, j), rows)]
        arrive = in_recv.at[j, s, t, k, bit_of(h, j)]
        if (dk, db) == (0, 0):
            return pltpu.make_async_copy(src, dst, arrive)
        return pltpu.make_async_remote_copy(
            src_ref=src, dst_ref=dst,
            send_sem=in_send.at[j, s, t, dk, db], recv_sem=arrive,
            device_id=dev(dk, db << j % 2), device_id_type=MESH,
        )

    def in_arrived(j, s, kk):
        for t in range(2):
            for b in range(2):
                dst = (q_buf, g_buf)[t].at[j, kk, s, pl.ds(b * rows, rows)]
                pltpu.make_async_copy(dst, dst, in_recv.at[j, s, t, kk, b]).wait()

    def up_copy(j, kk, dh):
        part = kv_buf.at[j, BACK + kk, :, at(flip(h, dh), rows)]
        return pltpu.make_async_remote_copy(
            src_ref=part, dst_ref=kv_buf.at[j, BACK + kk - 2, :, at(flip(h, dh), rows)],
            send_sem=up_send.at[j, kk, dh], recv_sem=up_recv.at[j, kk, dh],
            device_id=up, device_id_type=MESH,
        )

    def last_copy(j):
        return pltpu.make_async_remote_copy(
            src_ref=kv_buf.at[j, 2], dst_ref=kv_buf.at[j, 0],
            send_sem=last_send.at[j], recv_sem=last_recv.at[j],
            device_id=up, device_id_type=MESH,
        )

    def dq_copy(j, s, kk, b):
        src = dq_buf.at[j, kk, s, pl.ds(b * rows, rows)]
        dst = dq_out.at[:, at((SLOTS * j + mine[j]) * n_st + s, width)]
        arrive = dq_recv.at[j, s, k, bit_of(h, j)]
        shift = 1 << j % 2
        owner = h + shift * (b - bit_of(h, j))
        far = pltpu.make_async_remote_copy(
            src_ref=src, dst_ref=dst,
            send_sem=dq_send.at[j, s, kk, b], recv_sem=arrive,
            device_id=(2 * z + kk, owner), device_id_type=MESH,
        )
        own = pltpu.make_async_copy(src, dst, arrive)
        return far, own, (k == kk) & (bit_of(h, j) == b)

    def part_copy(j, m):
        return pltpu.make_async_remote_copy(
            src_ref=part_out.at[j, m], dst_ref=part_in.at[j, m],
            send_sem=part_send.at[j, m], recv_sem=part_recv.at[j, m],
            device_id=down, device_id_type=MESH,
        )

    def tot_copy(j, p):
        dk, dh = p
        return pltpu.make_async_remote_copy(
            src_ref=tot_out.at[j, flip(k, dk), :, at(flip(h, dh), rows)],
            dst_ref=tot_in.at[j, k, h],
            send_sem=tot_send.at[j, dk, dh], recv_sem=tot_recv.at[j, k, h],
            device_id=dev(dk, dh), device_id_type=MESH,
        )

    def start_kv(j):
        for p in plane:
            for t in range(2):
                kv_copy(j, t, p).start()

    def start_in(j, s):
        for db in range(2):
            for dk in range(2):
                for t in range(2):
                    in_copy(j, s, t, dk, db).start()

    start_kv(0)
    start_in(0, 0)
    for j in range(1, jobs):
        start_kv(j)
    for j in range(jobs):
        @pl.loop(1 if j == 0 else 0, n_st)
        def _(s):
            start_in(j, s)

    tile = HD
    lane = lax.broadcasted_iota(jnp.int32, (8, blk), 1)

    def make_bias(j, kk):
        shift = 1 << j % 2
        block = 2 * z + kk
        docs = jnp.broadcast_to(
            doc_ref[:, pl.ds(pl.multiple_of(block * blk, blk), blk)].astype(jnp.float32), (8, blk)
        )
        first = h - shift * bit_of(h, j)
        query_doc = jnp.zeros((8, blk), jnp.float32)
        for u in range(heads):
            for b in range(2):
                to = (2 * u + b) * rows
                turn = (to - (first + b * shift) * rows + 2 * blk) % blk
                query_doc = jnp.where(lane // rows == 2 * u + b, pltpu.roll(docs, turn, 1), query_doc)
        query_doc = query_doc[:1]
        col = lax.broadcasted_iota(jnp.int32, (tile, blk), 1)
        i = (first + (col // rows) % 2 * shift) * rows + col % rows
        for part in range(4 * blk // tile):
            key_blk = jnp.maximum(block - BACK + part * tile // blk, 0)
            start = pl.multiple_of(key_blk * blk + part * tile % blk, tile)
            key_row = doc_ref[:, pl.ds(start, tile)].astype(jnp.float32)
            key_doc = jnp.transpose(jnp.broadcast_to(key_row, (tile, tile)))
            key_doc = jnp.concatenate([key_doc] * (blk // tile), axis=1)
            row = lax.broadcasted_iota(jnp.int32, (tile, blk), 0) + part * tile
            ok = (row > i) & (row <= i + BACK * blk) & (row + (block - BACK) * blk >= 0)
            ok = ok & (key_doc == query_doc)
            bias[j, kk, pl.ds(part * tile, tile)] = jnp.where(ok, 0.0, -1e30)

    def gather_and_send_up(j):
        for dh in range(n_head):
            for dk in range(2):
                kv_arrived(j, (dk, dh))

            @pl.when(has_up)
            def _():
                for kk in (1, 0):
                    up_copy(j, kk, dh).start()

            yield

    def fill(j):
        @pl.when(z < 1)
        def _():
            kv_buf[j, 1:3] = jnp.zeros((2,) + kv_buf.shape[2:], kv_buf.dtype)

        @pl.when(z < 2)
        def _():
            kv_buf[j, 0] = jnp.zeros(kv_buf.shape[2:], kv_buf.dtype)

    def wait_down(j, kk):
        @pl.when(has_down)
        def _():
            for dh in range(n_head):
                up_copy(j, kk, dh).wait_recv()

    def hand_on(j):
        wait_down(j, 1)

        @pl.when(has_down & has_up)
        def _():
            last_copy(j).start()

    def wait_last(j):
        @pl.when(has_two)
        def _():
            last_copy(j).wait_recv()

    def turn_keys(j, first, last):
        keys = kv_buf[j, first:last, 0].reshape((last - first) * blk, HD)
        kt_buf[j, :, first * blk : last * blk] = jnp.transpose(keys.astype(jnp.float32)).astype(jnp.bfloat16)

    def attend(j, kk, s):
        in_arrived(j, s, kk)
        lanes = [slice(a * HD, (a + 1) * HD) for a in range(heads)]
        q = jnp.concatenate([q_buf[j, kk, s, :, a] for a in lanes], axis=0)
        g = jnp.concatenate([g_buf[j, kk, s, :, a] for a in lanes], axis=0)
        key_win = kv_buf[j, kk : kk + 4, 0].reshape(4 * blk, HD)
        val_win = kv_buf[j, kk : kk + 4, 1].reshape(4 * blk, HD)
        s_t = lax.dot_general(key_win, q, NT, preferred_element_type=jnp.float32)
        s_t = s_t + bias[j, kk]
        top = jnp.max(s_t, axis=0, keepdims=True)
        e_t = jnp.exp2((s_t - top) * (scale * math.log2(math.e)))
        w_t = e_t * (1.0 / jnp.sum(e_t, axis=0, keepdims=True))
        w_bf = w_t.astype(jnp.bfloat16)
        p_t = lax.dot_general(val_win, g, NT, preferred_element_type=jnp.float32)
        delta = jnp.sum(w_bf.astype(jnp.float32) * p_t, axis=0, keepdims=True)
        d_t = (w_t * (p_t - delta)).astype(jnp.bfloat16)
        dv = jnp.dot(w_bf, g, preferred_element_type=jnp.float32)
        dk = jnp.dot(d_t, q, preferred_element_type=jnp.float32)
        acc[j, kk : kk + 4, 0] += dk.reshape(4, blk, HD)
        acc[j, kk : kk + 4, 1] += dv.reshape(4, blk, HD)
        keys_t = kt_buf[j, :, kk * blk : (kk + 4) * blk]
        dq_t = jnp.dot(keys_t, d_t, preferred_element_type=jnp.float32)
        dq = jnp.transpose(dq_t * scale).astype(jnp.bfloat16)
        for n, a in enumerate(lanes):
            dq_buf[j, kk, s, :, a] = dq[n * pair : (n + 1) * pair]
        for b in range(2):
            far, own, here = dq_copy(j, s, kk, b)
            pl.when(jnp.logical_not(here))(far.start)
            pl.when(here)(own.start)

    def send_part(j, m, cond):
        part_out[j, m, 0] = (acc[j, m, 0] * scale).astype(jnp.bfloat16)
        part_out[j, m, 1] = acc[j, m, 1].astype(jnp.bfloat16)
        pl.when(cond)(part_copy(j, m).start)

    def add_part(j, m, cond):
        @pl.when(cond)
        def _():
            part_copy(j, m).wait_recv()
            acc[j, m + 2, 0] += part_in[j, m, 0].astype(jnp.float32) * (1.0 / scale)
            acc[j, m + 2, 1] += part_in[j, m, 1].astype(jnp.float32)

    def send_tot(j):
        for kk in range(2):
            add_part(j, kk + 1, has_up)
            tot_out[j, kk, 0] = (acc[j, BACK + kk, 0] * scale).astype(jnp.bfloat16)
            tot_out[j, kk, 1] = acc[j, BACK + kk, 1].astype(jnp.bfloat16)
        for p in others:
            tot_copy(j, p).start()
        tot_in[j, k, h] = tot_out[j, k, :, at(h, rows)]

    def send_mid(j):
        add_part(j, 0, has_up & has_down)
        send_part(j, 2, has_down)

    for j in range(jobs):
        fill(j)
        acc[j] = jnp.zeros(acc.shape[1:], acc.dtype)
    chores = [functools.partial(make_bias, j, kk) for j in range(jobs) for kk in (1, 0)]
    for _ in gather_and_send_up(0):
        if chores:
            chores.pop(0)()
    for chore in chores:
        chore()
    hand_on(0)

    for j in range(jobs):
        final = j == jobs - 1
        if j == 0:
            wait_down(0, 0)
            turn_keys(0, 1, 5)

            @pl.loop(0, n_st)
            def _(s):
                attend(0, 1, s)

                @pl.when(s == 0)
                def _():
                    if not final:
                        for _ in gather_and_send_up(1):
                            pass
                    wait_last(0)
                    turn_keys(0, 0, 1)

                attend(0, 0, s)

                if not final:
                    @pl.when(s == n_st // 2)
                    def _():
                        hand_on(1)
        else:
            wait_down(j, 0)
            wait_last(j)
            turn_keys(j, 0, 5)

            @pl.loop(0, n_st)
            def _(s):
                attend(j, 0, s)

                @pl.when(s == 0)
                def _():
                    send_mid(j - 1)
                    if not final:
                        for _ in gather_and_send_up(j + 1):
                            pass

            send_part(j, 0, has_two)

            @pl.loop(0, n_st)
            def _(s):
                attend(j, 1, s)

                @pl.when(s == 0)
                def _():
                    send_tot(j - 1)
                    if not final:
                        hand_on(j + 1)

        if j == 0:
            send_part(j, 0, has_two)
        send_part(j, 1, has_down)
        if final:
            send_mid(j)
            send_tot(j)

    for j in range(jobs):
        for b in range(2):
            for kk in range(2):
                n = SLOTS * j + 2 * b + kk
                for t in range(2):
                    total = jnp.zeros((rows, HD), jnp.float32)
                    for hh in range(n_head):
                        if (hh >> j % 2) & 1 == b:
                            if t == 0:
                                @pl.when((k != kk) | (h != hh))
                                def _():
                                    got = tot_in.at[j, kk, hh]
                                    pltpu.make_async_copy(got, got, tot_recv.at[j, kk, hh]).wait()
                            total = total + tot_in[j, kk, hh, t].astype(jnp.float32)
                    (dk_out, dv_out)[t][:, n * HD : (n + 1) * HD] = total

    for j in range(jobs):
        @pl.loop(0, n_st)
        def _(s):
            for dk in range(2):
                for b in range(2):
                    if (dk, b) != (0, 0):
                        for t in range(2):
                            in_copy(j, s, t, dk, b).wait_send()
                    far, own, here = dq_copy(j, s, dk, b)
                    pl.when(jnp.logical_not(here))(far.wait_send)
                    got = dq_buf.at[j, dk, s, pl.ds(b * rows, rows)]
                    pltpu.make_async_copy(got, got, dq_recv.at[j, s, dk, b]).wait()

        for p in others:
            for t in range(2):
                kv_copy(j, t, p).wait_send()
            tot_copy(j, p).wait_send()

        @pl.when(has_up)
        def _():
            for kk in range(2):
                for dh in range(n_head):
                    up_copy(j, kk, dh).wait_send()

        pl.when(has_up & has_down)(last_copy(j).wait_send)
        pl.when(has_two)(part_copy(j, 0).wait_send)
        pl.when(has_down)(part_copy(j, 1).wait_send)
        pl.when(has_down)(part_copy(j, 2).wait_send)


def body(queries, keys, values, out_grad, doc_ids):
    n_ctx, n_head = lax.axis_size("ctx"), lax.axis_size("head")
    rows, q_cols = queries.shape
    kv_cols = keys.shape[1]
    blk = rows * n_head
    jobs = kv_cols // HD // SLOTS
    group = q_cols // kv_cols
    heads = n_head // 2
    n_st = group // heads
    pair = 2 * rows
    win = BACK + 2
    bf, f32, dma = jnp.bfloat16, jnp.float32, pltpu.SemaphoreType.DMA
    far = pl.BlockSpec(memory_space=pl.ANY)
    near = pl.BlockSpec(memory_space=pltpu.VMEM)
    dq, dk, dv = pl.pallas_call(
        functools.partial(kernel, n_ctx, n_head),
        out_shape=(
            jax.ShapeDtypeStruct((rows, q_cols), bf),
            jax.ShapeDtypeStruct((rows, kv_cols), f32),
            jax.ShapeDtypeStruct((rows, kv_cols), f32),
        ),
        in_specs=[far, far, far, far, near],
        out_specs=(far, near, near),
        scratch_shapes=[
            pltpu.VMEM((jobs, 2, n_st, pair, heads * HD), bf),
            pltpu.VMEM((jobs, 2, n_st, pair, heads * HD), bf),
            pltpu.VMEM((jobs, 2, n_st, pair, heads * HD), bf),
            pltpu.VMEM((jobs, win, 2, blk, HD), bf),
            pltpu.VMEM((jobs, HD, win * blk), bf),
            pltpu.VMEM((jobs, win, 2, blk, HD), f32),
            pltpu.VMEM((jobs, 2, 4 * blk, blk), f32),
            pltpu.VMEM((jobs, 3, 2, blk, HD), bf),
            pltpu.VMEM((jobs, 3, 2, blk, HD), bf),
            pltpu.VMEM((jobs, 2, 2, blk, HD), bf),
            pltpu.VMEM((jobs, 2, n_head, 2, rows, HD), bf),
            dma((jobs, 2, 2, n_head)),
            dma((jobs, 2, 2, n_head)),
            dma((jobs, n_st, 2, 2, 2)),
            dma((jobs, n_st, 2, 2, 2)),
            dma((jobs, 2, n_head)),
            dma((jobs, 2, n_head)),
            dma((jobs,)),
            dma((jobs,)),
            dma((jobs, n_st, 2, 2)),
            dma((jobs, n_st, 2, 2)),
            dma((jobs, 3)),
            dma((jobs, 3)),
            dma((jobs, 2, n_head)),
            dma((jobs, 2, n_head)),
        ],
        compiler_params=pltpu.CompilerParams(
            collective_id=0, has_side_effects=True, vmem_limit_bytes=56 * 2**20
        ),
    )(queries, keys, values, out_grad, doc_ids.reshape(1, -1))
    return dq.astype(f32), dk, dv


def solution(mesh):
    split = P(("ctx", "head"), None)
    return jax.shard_map(
        body,
        mesh=mesh,
        in_specs=(split, split, split, split, P()),
        out_specs=(split, split, split),
        check_vma=False,
    )
```

```python
import functools
import math
import jax
import jax.numpy as jnp
from jax import lax
from jax.experimental import pallas as pl
from jax.experimental.pallas import tpu as pltpu
from jax.sharding import PartitionSpec as P

HD = 128
BACK = 3
SLOTS = 4
CUTS = 8
MESH = pl.DeviceIdType.MESH
NT = (((1,), (1,)), ((), ()))


def flip(v, mask):
    bit = 1
    while bit <= mask:
        if mask & bit:
            v = v + bit * (1 - 2 * ((v // bit) % 2))
        bit *= 2
    return v


def kernel(
    n_ctx, n_head,
    q_ref, k_ref, v_ref, g_ref, doc_ref,
    dq_out, dk_out, dv_out,
    own_buf, qg_buf, dq_buf, kv_buf, kt_buf, acc, bias, red_out, red_in, part_out, tot_in,
    s_buf, p_buf, w_buf, d_buf,
    own_sem, kv_send, kv_recv, in_send, in_recv, up_send, up_recv, last_send, last_recv,
    dq_send, dq_recv, red_send, red_recv, part_send, tot_send, tot_recv,
):
    c = lax.axis_index("ctx")
    h = lax.axis_index("head")
    k = c % 2
    z = c // 2
    n_z = n_ctx // 2
    rows = q_ref.shape[0]
    blk = rows * n_head
    jobs, _, n_st, _, pair, width = qg_buf.shape
    heads = width // HD
    scale = 1.0 / HD**0.5
    has_up, has_down, has_two = z + 1 < n_z, z >= 1, z >= 2

    def at(n, size):
        return pl.ds(pl.multiple_of(n * size, size), size)

    def bit_of(v, j):
        return (v // (1 << j % 2)) % 2

    def dev(dk, dh):
        return (flip(c, dk), flip(h, dh))

    mine = [2 * bit_of(h, j) + k for j in range(jobs)]
    plane = [(dk, dh) for dh in range(n_head) for dk in range(2)]
    others = plane[1:]
    up = ((c + 2) % n_ctx, h)
    down = ((c - 2 + n_ctx) % n_ctx, h)

    def masks(j):
        return [m for m in range(1, n_head) if not m >> j % 2 & 1]

    def place(v, j):
        bit = 1 << j % 2
        return v % bit + v // (2 * bit) * bit

    def head_of(b, o, j):
        bit = 1 << j % 2
        return o % bit + b * bit + o // bit * 2 * bit


    barrier = pltpu.get_barrier_semaphore()
    for to in [dev(*p) for p in others] + [up, down]:
        pl.semaphore_signal(barrier, inc=1, device_id=to, device_id_type=MESH)

    for j in range(jobs):
        for b in range(2):
            for core in range(2):
                head = head_of(b, h // 2, j)
                above = (2 * z + 2 + core) % n_ctx
                pl.semaphore_signal(barrier, inc=1, device_id=(above, head), device_id_type=MESH)

                @pl.when(k == 1)
                def _():
                    far = (2 * z + 4 + core) % n_ctx
                    pl.semaphore_signal(barrier, inc=1, device_id=(far, head), device_id_type=MESH)
    for t in range(2):
        pltpu.make_async_copy((k_ref, v_ref)[t], own_buf.at[t], own_sem.at[t]).start()

    def kv_copy(j, t, p):
        dk, dh = p
        slot = 2 * bit_of(flip(h, dh), j) + flip(k, dk)
        src = own_buf.at[t, :, at(SLOTS * j + slot, HD)]
        dst = kv_buf.at[j, BACK + k, t, at(h, rows)]
        return pltpu.make_async_remote_copy(
            src_ref=src, dst_ref=dst,
            send_sem=kv_send.at[j, dh], recv_sem=kv_recv.at[j, dh],
            device_id=dev(dk, dh), device_id_type=MESH,
        )

    def await_bytes(ref, sem):
        pltpu.make_async_copy(ref, ref, sem).wait()

    def kv_arrived(j, dh):
        if dh == 0:
            await_bytes(kv_buf.at[j, BACK, :, at(h, rows)], kv_recv.at[j, 0])
            for t in range(2):
                kv_buf[j, BACK + k, t, at(h, rows)] = own_buf[t, :, at(SLOTS * j + mine[j], HD)]
        else:
            await_bytes(kv_buf.at[j, BACK : BACK + 2, :, at(flip(h, dh), rows)], kv_recv.at[j, dh])

    def in_copy(j, s, t, dk, db):
        slot = 2 * flip(bit_of(h, j), db) + flip(k, dk)
        src = (q_ref, g_ref)[t].at[:, at((SLOTS * j + slot) * n_st + s, width)]
        dst = qg_buf.at[j, k, s, t, at(bit_of(h, j), rows)]
        arrive = in_recv.at[j, s, k]
        if (dk, db) == (0, 0):
            return pltpu.make_async_copy(src, dst, arrive)
        return pltpu.make_async_remote_copy(
            src_ref=src, dst_ref=dst,
            send_sem=in_send.at[j, db], recv_sem=arrive,
            device_id=dev(dk, db << j % 2), device_id_type=MESH,
        )

    def in_arrived(j, s, kk):
        await_bytes(qg_buf.at[j, kk, s], in_recv.at[j, s, kk])

    def up_copy(j, kk, dh):
        part = kv_buf.at[j, BACK + kk, :, at(flip(h, dh), rows)]
        return pltpu.make_async_remote_copy(
            src_ref=part, dst_ref=kv_buf.at[j, BACK + kk - 2, :, at(flip(h, dh), rows)],
            send_sem=up_send.at[j], recv_sem=up_recv.at[j, kk, dh],
            device_id=up, device_id_type=MESH,
        )

    def last_copy(j, dh):
        return pltpu.make_async_remote_copy(
            src_ref=kv_buf.at[j, 2, :, at(flip(h, dh), rows)], dst_ref=kv_buf.at[j, 0, :, at(flip(h, dh), rows)],
            send_sem=last_send.at[j], recv_sem=last_recv.at[j],
            device_id=up, device_id_type=MESH,
        )

    def dq_send_out(j, s, kk):
        for b in range(2):
            src = dq_buf.at[j, kk, s, pl.ds(b * rows, rows)]
            dst = dq_out.at[:, at((SLOTS * j + mine[j]) * n_st + s, width)]
            here = (k == kk) & (bit_of(h, j) == b)

            @pl.when(jnp.logical_not(here))
            def _():
                pltpu.make_async_remote_copy(
                    src_ref=src, dst_ref=dst,
                    send_sem=dq_send.at[j, (k + kk) % 2], recv_sem=dq_recv.at[j],
                    device_id=(2 * z + kk, h + (1 << j % 2) * (b - bit_of(h, j))), device_id_type=MESH,
                ).start()

            @pl.when(here)
            def _():
                pltpu.make_async_copy(src, dst, dq_recv.at[j]).start()

    def red_copy(j, i, n):
        mask = masks(j)[n]
        return pltpu.make_async_remote_copy(
            src_ref=red_out.at[j, i, :, at(place(flip(h, mask), j), pair)], dst_ref=red_in.at[j, i, n],
            send_sem=red_send.at[j, i], recv_sem=red_recv.at[j, i],
            device_id=(c, flip(h, mask)), device_id_type=MESH,
        )

    group = n_head // 2

    def part_copy(j, i, e):
        return pltpu.make_async_remote_copy(
            src_ref=part_out.at[j, i, :, pl.ds(e * rows, rows)],
            dst_ref=tot_in.at[j, mine[j], group + (1 if i == 0 else 0)],
            send_sem=part_send.at[j, i, e], recv_sem=tot_recv.at[j, mine[j], group + (1 if i == 0 else 0)],
            device_id=((2 * z - BACK + i + n_ctx) % n_ctx, 2 * place(h, j) + e), device_id_type=MESH,
        )

    def tot_copy(j, p):
        dk, dh = p
        return pltpu.make_async_remote_copy(
            src_ref=red_out.at[j, BACK + flip(k, dk), :, at(flip(h, dh), rows)],
            dst_ref=tot_in.at[j, mine[j], place(h, j)],
            send_sem=tot_send.at[j, dk, dh], recv_sem=tot_recv.at[j, mine[j], place(h, j)],
            device_id=dev(dk, dh), device_id_type=MESH,
        )

    def start_kv(j):
        for p in others:
            for t in range(2):
                kv_copy(j, t, p).start()

    def start_in(j, s):
        for db in range(2):
            for dk in range(2):
                for t in range(2):
                    in_copy(j, s, t, dk, db).start()

    tile = HD
    lane = lax.broadcasted_iota(jnp.int32, (8, blk), 1)

    def make_bias(j, kk):
        shift = 1 << j % 2
        block = 2 * z + kk
        docs = jnp.broadcast_to(
            doc_ref[:, pl.ds(pl.multiple_of(block * blk, blk), blk)].astype(jnp.float32), (8, blk)
        )
        first = h - shift * bit_of(h, j)
        query_doc = jnp.zeros((8, blk), jnp.float32)
        for u in range(heads):
            for b in range(2):
                to = (2 * u + b) * rows
                turn = (to - (first + b * shift) * rows + 2 * blk) % blk
                query_doc = jnp.where(lane // rows == 2 * u + b, pltpu.roll(docs, turn, 1), query_doc)
        query_doc = query_doc[:1]
        col = lax.broadcasted_iota(jnp.int32, (tile, blk), 1)
        i = (first + (col // rows) % 2 * shift) * rows + col % rows
        for part in range(4 * blk // tile):
            key_blk = jnp.maximum(block - BACK + part * tile // blk, 0)
            start = pl.multiple_of(key_blk * blk + part * tile % blk, tile)
            key_row = doc_ref[:, pl.ds(start, tile)].astype(jnp.float32)
            key_doc = jnp.transpose(jnp.broadcast_to(key_row, (tile, tile)))
            key_doc = jnp.concatenate([key_doc] * (blk // tile), axis=1)
            row = lax.broadcasted_iota(jnp.int32, (tile, blk), 0) + part * tile
            ok = (row > i) & (row <= i + BACK * blk) & (row + (block - BACK) * blk >= 0)
            ok = ok & (key_doc == query_doc)
            bias[j, kk, pl.ds(part * tile, tile)] = jnp.where(ok, 0.0, -1e30)

    def gather_and_send_up(j):
        for dh in range(n_head):
            kv_arrived(j, dh)

            @pl.when(has_up)
            def _():
                for kk in (1, 0):
                    up_copy(j, kk, dh).start()

            yield

    def fill(j):
        @pl.when(z < 1)
        def _():
            kv_buf[j, 1:3] = jnp.zeros((2,) + kv_buf.shape[2:], kv_buf.dtype)

        @pl.when(z < 2)
        def _():
            kv_buf[j, 0] = jnp.zeros(kv_buf.shape[2:], kv_buf.dtype)

    def wait_down(j):
        @pl.when(has_down)
        def _():
            for dh in range(n_head):
                await_bytes(kv_buf.at[j, 1, :, at(flip(h, dh), rows)], up_recv.at[j, 0, dh])

    def hand_on(j):
        @pl.when(has_down)
        def _():
            for dh in range(n_head):
                await_bytes(kv_buf.at[j, 2, :, at(flip(h, dh), rows)], up_recv.at[j, 1, dh])
                pl.when(has_up)(last_copy(j, dh).start)

    def wait_last(j):
        @pl.when(has_two)
        def _():
            await_bytes(kv_buf.at[j, 0], last_recv.at[j])

    def turn_keys(j, first, last):
        keys = kv_buf[j, first:last, 0].reshape((last - first) * blk, HD)
        kt_buf[j, :, first * blk : last * blk] = jnp.transpose(keys.astype(jnp.float32)).astype(jnp.bfloat16)

    lanes = [slice(a * HD, (a + 1) * HD) for a in range(heads)]
    log_scale = scale * math.log2(math.e)
    fine = 32
    tiles = 4 * blk // fine

    def stacked(j, kk, s, t):
        return jnp.concatenate([qg_buf[j, kk, s, t, :, a] for a in lanes], axis=0)

    def fold(x, op):
        return op(x.reshape(x.shape[0] // 8, 8, blk), axis=0)

    def scores(step, slot, made):
        j, kk, s = step
        q, g = stacked(j, kk, s, 0), stacked(j, kk, s, 1)
        high = None
        for n in range(4):
            s_t = lax.dot_general(kv_buf[j, kk + n, 0], q, NT, preferred_element_type=jnp.float32)
            p_t = lax.dot_general(kv_buf[j, kk + n, 1], g, NT, preferred_element_type=jnp.float32)
            for m in range(blk // fine):
                span, part = pl.ds(n * blk + m * fine, fine), slice(m * fine, (m + 1) * fine)
                one = s_t[part] + bias[j, kk, span]
                s_buf[slot][span] = one
                p_buf[slot][span] = p_t[part]
                one = fold(one, jnp.max)
                high = one if high is None else jnp.maximum(high, one)
                yield
        made["top"] = jnp.max(high, axis=0, keepdims=True)

    def exponentials(slot, made):
        top = made["top"]
        total = None
        for n in range(tiles):
            span = pl.ds(n * fine, fine)
            e_t = jnp.exp2((s_buf[slot][span] - top) * log_scale)
            s_buf[slot][span] = e_t
            one = fold(e_t, jnp.sum)
            total = one if total is None else total + one
            yield
        made["inverse"] = 1.0 / jnp.sum(total, axis=0, keepdims=True)

    def weights(slot, to, made):
        inverse = made["inverse"]
        total = None
        for n in range(tiles):
            span = pl.ds(n * fine, fine)
            w_t = s_buf[slot][span] * inverse
            s_buf[slot][span] = w_t
            w_bf = w_t.astype(jnp.bfloat16)
            w_buf[to][span] = w_bf
            one = fold(w_bf.astype(jnp.float32) * p_buf[slot][span], jnp.sum)
            total = one if total is None else total + one
            yield
        made["delta"] = jnp.sum(total, axis=0, keepdims=True)

    def differences(slot, to, made):
        delta = made["delta"]
        for n in range(tiles):
            span = pl.ds(n * fine, fine)
            d_buf[to][span] = (s_buf[slot][span] * (p_buf[slot][span] - delta)).astype(jnp.bfloat16)
            yield

    def gradients(step, slot, slot_w):
        j, kk, s = step
        q, g = stacked(j, kk, s, 0), stacked(j, kk, s, 1)
        for n in range(4):
            span = pl.ds(n * blk, blk)
            for t, left, right in ((1, w_buf[slot_w], g), (0, d_buf[slot], q)):
                more = jnp.dot(left[span], right, preferred_element_type=jnp.float32)
                for m in range(0, blk, 2 * fine):
                    acc[j, kk + n, t, pl.ds(m, 2 * fine)] += more[m : m + 2 * fine]
                    yield
        keys_t = kt_buf[j, :, kk * blk : (kk + 4) * blk]
        dq_t = jnp.dot(keys_t, d_buf[slot][...], preferred_element_type=jnp.float32)
        dq = jnp.transpose(dq_t * scale).astype(jnp.bfloat16)
        for n, a in enumerate(lanes):
            dq_buf[j, kk, s, :, a] = dq[n * pair : (n + 1) * pair]

    def in_turns(pieces):
        pieces = list(pieces)
        while pieces:
            pieces = [p for p in pieces if next(p, "end") != "end"]

    need = (has_two, has_down, has_down)

    def round_out(j, i):
        red_out[j, i, 0] = (acc[j, i, 0] * scale).astype(jnp.bfloat16)
        red_out[j, i, 1] = acc[j, i, 1].astype(jnp.bfloat16)

    def share(j, i):
        round_out(j, i)

        @pl.when(need[i])
        def _():
            for n in range(len(masks(j))):
                red_copy(j, i, n).start()

    def send_part(j, i):
        @pl.when(need[i])
        def _():
            await_bytes(red_in.at[j, i], red_recv.at[j, i])
            mine_here = at(place(h, j), pair)
            sums = [acc[j, i, 0, mine_here] * scale, acc[j, i, 1, mine_here]]
            for t in range(2):
                for n in range(len(masks(j))):
                    sums[t] = sums[t] + red_in[j, i, n, t].astype(jnp.float32)
                part_out[j, i, t] = sums[t].astype(jnp.bfloat16)
            for e in range(2):
                part_copy(j, i, e).start()

    def send_own(j):
        for kk in range(2):
            round_out(j, BACK + kk)
        for p in others:
            tot_copy(j, p).start()
        tot_in[j, mine[j], place(h, j)] = red_out[j, BACK + k, :, at(h, rows)]

    for j in range(jobs):
        fill(j)
        acc[j] = jnp.zeros(acc.shape[1:], acc.dtype)
        for kk in range(2):
            make_bias(j, kk)

    pl.semaphore_wait(barrier, len(others) + 2 + 6 * jobs)
    for t in range(2):
        await_bytes(own_buf.at[t], own_sem.at[t])
    start_kv(0)
    start_in(0, 0)
    start_in(0, 1)
    for j in range(1, jobs):
        start_kv(j)
    for j in range(jobs):
        @pl.loop(2 if j == 0 else 0, n_st)
        def _(s):
            start_in(j, s)

    for _ in gather_and_send_up(0):
        pass
    hand_on(0)
    wait_down(0)
    turn_keys(0, 1, 5)

    steps = []
    half = n_st // 2
    for j in range(jobs):
        if j == 0:
            order = [(kk, s) for kk in (1, 0) for s in range(half)] + [(kk, s) for s in range(half, n_st) for kk in (1, 0)]
        else:
            order = [(1, s) for s in range(half)] + [(0, s) for s in range(n_st)] + [(1, s) for s in range(half, n_st)]
        steps += [(j, kk, s) for kk, s in order]
    per_job = 2 * n_st

    def before(n):
        j, first = n // per_job, n % per_job
        if j > 0 and first == 0:
            wait_down(j)
            turn_keys(j, 1, 5)
        if first == half:
            wait_last(j)
            turn_keys(j, 0, 1)
        if first == 1 and j + 1 < jobs:
            for _ in gather_and_send_up(j + 1):
                pass
        if first == per_job - 2 and j + 1 < jobs:
            hand_on(j + 1)
        in_arrived(*steps[n][:1], steps[n][2], steps[n][1])

    def after(n):
        j, first = n // per_job, n % per_job
        dq_send_out(j, steps[n][2], steps[n][1])
        last = j == jobs - 1
        if j > 0 and first == per_job // 2:
            send_part(j - 1, 0)
            send_part(j - 1, 1)
        if j > 0 and first == half + n_st - 1:
            share(j, 0)
        if j > 0 and first == per_job - 2:
            send_part(j - 1, 2)
        if first == per_job - 1:
            for i in range(1 if j > 0 else 0, BACK):
                share(j, i)
            send_own(j)
            if last:
                for i in range(BACK):
                    send_part(j, i)

    made = [{} for _ in steps]
    for n in range(len(steps) + 4):
        pieces = []
        if n < len(steps):
            before(n)
        if 0 <= n - 4:
            pieces.append(gradients(steps[n - 4], n % 2, (n - 4) % 3))
        if n < len(steps):
            pieces.append(scores(steps[n], n % 4, made[n]))
        if 0 <= n - 1 < len(steps):
            pieces.append(exponentials((n - 1) % 4, made[n - 1]))
        if 0 <= n - 2 < len(steps):
            pieces.append(weights((n - 2) % 4, (n - 2) % 3, made[n - 2]))
        if 0 <= n - 3 < len(steps):
            pieces.append(differences((n - 3) % 4, (n - 3) % 2, made[n - 3]))
        in_turns(pieces)
        if 0 <= n - 4:
            after(n - 4)

    for j in range(jobs):
        for slot in range(SLOTS):
            n = SLOTS * j + slot
            for o in range(group):
                @pl.when((mine[j] != slot) | (place(h, j) != o))
                def _():
                    await_bytes(tot_in.at[j, slot, o], tot_recv.at[j, slot, o])

            for far, cond in ((0, has_up), (1, (z + 2 < n_z) & (k == 1))):
                @pl.when(cond)
                def _():
                    await_bytes(tot_in.at[j, slot, group + far], tot_recv.at[j, slot, group + far])

                @pl.when(jnp.logical_not(cond))
                def _():
                    tot_in[j, slot, group + far] = jnp.zeros(tot_in.shape[3:], tot_in.dtype)

            for t in range(2):
                total = tot_in[j, slot, 0, t].astype(jnp.float32)
                for o in range(1, group + 2):
                    total = total + tot_in[j, slot, o, t].astype(jnp.float32)
                (dk_out, dv_out)[t][:, n * HD : (n + 1) * HD] = total

    for j in range(jobs):
        await_bytes(dq_buf.at[j, 0], in_send.at[j, 0])
        await_bytes(qg_buf.at[j, 0], in_send.at[j, 1])
        await_bytes(dq_buf.at[j, 0, :, pl.ds(0, rows)], dq_send.at[j, 0])
        await_bytes(dq_buf.at[j, 0], dq_send.at[j, 1])
        await_bytes(qg_buf.at[j, 0], dq_recv.at[j])
        await_bytes(kv_buf.at[j, 0, :, pl.ds(0, rows)], kv_send.at[j, 0])
        for dh in range(1, n_head):
            await_bytes(kv_buf.at[j, 0:2, :, pl.ds(0, rows)], kv_send.at[j, dh])
        for p in others:
            tot_copy(j, p).wait_send()

        for i in range(BACK):
            @pl.when(need[i])
            def _():
                await_bytes(red_in.at[j, i], red_send.at[j, i])
                for e in range(2):
                    part_copy(j, i, e).wait_send()

        @pl.when(has_up)
        def _():
            await_bytes(kv_buf.at[j, 0:2], up_send.at[j])

        @pl.when(has_up & has_down)
        def _():
            await_bytes(kv_buf.at[j, 0], last_send.at[j])


def widen(*refs):
    src, dst, near, wide, (get, put) = refs[:3], refs[3:6], refs[6:9], refs[9:12], refs[12:]
    step = src[0].shape[1] // CUTS
    pieces = [(0, pl.ds(n * step, step)) for n in range(CUTS)] + [(n, pl.ds(0, src[n].shape[1])) for n in (1, 2)]
    reads = [pltpu.make_async_copy(src[a].at[:, s], near[a].at[:, s], get.at[n]) for n, (a, s) in enumerate(pieces)]
    writes = [pltpu.make_async_copy(wide[a].at[:, s], dst[a].at[:, s], put.at[n]) for n, (a, s) in enumerate(pieces)]
    for read in reads:
        read.start()
    for (a, s), read, write in zip(pieces, reads, writes):
        read.wait()
        wide[a][:, s] = near[a][:, s].astype(jnp.float32)
        write.start()
    for write in writes:
        write.wait()


def body(queries, keys, values, out_grad, doc_ids):
    n_ctx, n_head = lax.axis_size("ctx"), lax.axis_size("head")
    rows, q_cols = queries.shape
    kv_cols = keys.shape[1]
    blk = rows * n_head
    jobs = kv_cols // HD // SLOTS
    group = q_cols // kv_cols
    heads = n_head // 2
    n_st = group // heads
    pair = 2 * rows
    win = BACK + 2
    bf, f32, dma = jnp.bfloat16, jnp.float32, pltpu.SemaphoreType.DMA
    far = pl.BlockSpec(memory_space=pl.ANY)
    near = pl.BlockSpec(memory_space=pltpu.VMEM)
    dq, dk, dv = pl.pallas_call(
        functools.partial(kernel, n_ctx, n_head),
        out_shape=(
            jax.ShapeDtypeStruct((rows, q_cols), bf),
            jax.ShapeDtypeStruct((rows, kv_cols), f32),
            jax.ShapeDtypeStruct((rows, kv_cols), f32),
        ),
        in_specs=[far, far, far, far, near],
        out_specs=(far, near, near),
        scratch_shapes=[
            pltpu.VMEM((2, rows, kv_cols), bf),
            pltpu.VMEM((jobs, 2, n_st, 2, pair, heads * HD), bf),
            pltpu.VMEM((jobs, 2, n_st, pair, heads * HD), bf),
            pltpu.VMEM((jobs, win, 2, blk, HD), bf),
            pltpu.VMEM((jobs, HD, win * blk), bf),
            pltpu.VMEM((jobs, win, 2, blk, HD), f32),
            pltpu.VMEM((jobs, 2, 4 * blk, blk), f32),
            pltpu.VMEM((jobs, win, 2, blk, HD), bf),
            pltpu.VMEM((jobs, BACK, n_head // 2 - 1, 2, pair, HD), bf),
            pltpu.VMEM((jobs, BACK, 2, pair, HD), bf),
            pltpu.VMEM((jobs, SLOTS, n_head // 2 + 2, 2, rows, HD), bf),
            (pltpu.VMEM((4 * blk, blk), f32),) * 4,
            (pltpu.VMEM((4 * blk, blk), f32),) * 4,
            (pltpu.VMEM((4 * blk, blk), bf),) * 3,
            (pltpu.VMEM((4 * blk, blk), bf),) * 2,
            dma((2,)),
            dma((jobs, n_head)),
            dma((jobs, n_head)),
            dma((jobs, 2)),
            dma((jobs, n_st, 2)),
            dma((jobs,)),
            dma((jobs, 2, n_head)),
            dma((jobs,)),
            dma((jobs,)),
            dma((jobs, 2)),
            dma((jobs,)),
            dma((jobs, BACK)),
            dma((jobs, BACK)),
            dma((jobs, BACK, 2)),
            dma((jobs, 2, n_head)),
            dma((jobs, SLOTS, n_head // 2 + 2)),
        ],
        compiler_params=pltpu.CompilerParams(
            collective_id=0, has_side_effects=True, vmem_limit_bytes=56 * 2**20
        ),
    )(queries, keys, values, out_grad, doc_ids.reshape(1, -1))
    outs = [jax.ShapeDtypeStruct(x.shape, f32) for x in (dq, dk, dv)]
    return pl.pallas_call(
        widen,
        out_shape=outs,
        in_specs=[far] * 3,
        out_specs=[far] * 3,
        scratch_shapes=[
            *[pltpu.VMEM(x.shape, x.dtype) for x in (dq, dk, dv)],
            *[pltpu.VMEM(x.shape, f32) for x in (dq, dk, dv)],
            dma((CUTS + 2,)),
            dma((CUTS + 2,)),
        ],
    )(dq, dk, dv)


def solution(mesh):
    split = P(("ctx", "head"), None)
    return jax.shard_map(
        body,
        mesh=mesh,
        in_specs=(split, split, split, split, P()),
        out_specs=(split, split, split),
        check_vma=False,
    )
```

```python
import functools
import math
import jax
import jax.numpy as jnp
from jax import lax
from jax.experimental import pallas as pl
from jax.experimental.pallas import tpu as pltpu
from jax.sharding import PartitionSpec as P

HD = 128
BACK = 3
SLOTS = 4
CUTS = 8
MESH = pl.DeviceIdType.MESH
NT = (((1,), (1,)), ((), ()))


def flip(v, mask):
    bit = 1
    while bit <= mask:
        if mask & bit:
            v = v + bit * (1 - 2 * ((v // bit) % 2))
        bit *= 2
    return v


def kernel(
    n_ctx, n_head,
    q_ref, k_ref, v_ref, g_ref, doc_ref,
    dq_out, dk_out, dv_out,
    own_buf, qg_buf, dq_buf, kv_buf, kt_buf, acc, bias, red_out, red_in, part_out, tot_in,
    s_buf, p_buf, w_buf, d_buf,
    own_sem, kv_send, kv_recv, in_send, in_recv, up_send, up_recv, last_send, last_recv,
    dq_send, dq_recv, red_send, red_recv, part_send, tot_send, tot_recv,
):
    c = lax.axis_index("ctx")
    h = lax.axis_index("head")
    k = c % 2
    z = c // 2
    n_z = n_ctx // 2
    rows = q_ref.shape[0]
    blk = rows * n_head
    jobs, _, n_st, _, pair, width = qg_buf.shape
    heads = width // HD
    scale = 1.0 / HD**0.5
    has_up, has_down, has_two = z + 1 < n_z, z >= 1, z >= 2

    def at(n, size):
        return pl.ds(pl.multiple_of(n * size, size), size)

    def bit_of(v, j):
        return (v // (1 << j % 2)) % 2

    def dev(dk, dh):
        return (flip(c, dk), flip(h, dh))

    mine = [2 * bit_of(h, j) + k for j in range(jobs)]
    plane = [(dk, dh) for dh in range(n_head) for dk in range(2)]
    others = plane[1:]
    up = ((c + 2) % n_ctx, h)
    down = ((c - 2 + n_ctx) % n_ctx, h)

    def masks(j):
        return [m for m in range(1, n_head) if not m >> j % 2 & 1]

    def place(v, j):
        bit = 1 << j % 2
        return v % bit + v // (2 * bit) * bit

    def head_of(b, o, j):
        bit = 1 << j % 2
        return o % bit + b * bit + o // bit * 2 * bit


    barrier = pltpu.get_barrier_semaphore()
    for to in [dev(*p) for p in others] + [up, down]:
        pl.semaphore_signal(barrier, inc=1, device_id=to, device_id_type=MESH)

    for j in range(jobs):
        for b in range(2):
            for core in range(2):
                head = head_of(b, h // 2, j)
                above = (2 * z + 2 + core) % n_ctx
                pl.semaphore_signal(barrier, inc=1, device_id=(above, head), device_id_type=MESH)

                @pl.when(k == 1)
                def _():
                    far = (2 * z + 4 + core) % n_ctx
                    pl.semaphore_signal(barrier, inc=1, device_id=(far, head), device_id_type=MESH)
    for t in range(2):
        pltpu.make_async_copy((k_ref, v_ref)[t], own_buf.at[t], own_sem.at[t]).start()

    def kv_copy(j, t, p):
        dk, dh = p
        slot = 2 * bit_of(flip(h, dh), j) + flip(k, dk)
        src = own_buf.at[t, :, at(SLOTS * j + slot, HD)]
        dst = kv_buf.at[j, BACK + k, t, at(h, rows)]
        return pltpu.make_async_remote_copy(
            src_ref=src, dst_ref=dst,
            send_sem=kv_send.at[j, dh], recv_sem=kv_recv.at[j, dh],
            device_id=dev(dk, dh), device_id_type=MESH,
        )

    def await_bytes(ref, sem):
        pltpu.make_async_copy(ref, ref, sem).wait()

    def kv_arrived(j, dh):
        if dh == 0:
            await_bytes(kv_buf.at[j, BACK, :, at(h, rows)], kv_recv.at[j, 0])
            for t in range(2):
                kv_buf[j, BACK + k, t, at(h, rows)] = own_buf[t, :, at(SLOTS * j + mine[j], HD)]
        else:
            await_bytes(kv_buf.at[j, BACK : BACK + 2, :, at(flip(h, dh), rows)], kv_recv.at[j, dh])

    def in_copy(j, s, t, dk, db):
        slot = 2 * flip(bit_of(h, j), db) + flip(k, dk)
        src = (q_ref, g_ref)[t].at[:, at((SLOTS * j + slot) * n_st + s, width)]
        dst = qg_buf.at[j, k, s, t, at(bit_of(h, j), rows)]
        arrive = in_recv.at[j, s, k]
        if (dk, db) == (0, 0):
            return pltpu.make_async_copy(src, dst, arrive)
        return pltpu.make_async_remote_copy(
            src_ref=src, dst_ref=dst,
            send_sem=in_send.at[j, db], recv_sem=arrive,
            device_id=dev(dk, db << j % 2), device_id_type=MESH,
        )

    def in_arrived(j, s, kk):
        await_bytes(qg_buf.at[j, kk, s], in_recv.at[j, s, kk])

    def up_copy(j, kk, dh):
        part = kv_buf.at[j, BACK + kk, :, at(flip(h, dh), rows)]
        return pltpu.make_async_remote_copy(
            src_ref=part, dst_ref=kv_buf.at[j, BACK + kk - 2, :, at(flip(h, dh), rows)],
            send_sem=up_send.at[j], recv_sem=up_recv.at[j, kk, dh],
            device_id=up, device_id_type=MESH,
        )

    def last_copy(j, dh):
        return pltpu.make_async_remote_copy(
            src_ref=kv_buf.at[j, 2, :, at(flip(h, dh), rows)], dst_ref=kv_buf.at[j, 0, :, at(flip(h, dh), rows)],
            send_sem=last_send.at[j], recv_sem=last_recv.at[j],
            device_id=up, device_id_type=MESH,
        )

    def dq_send_out(j, s, kk):
        for b in range(2):
            src = dq_buf.at[j, kk, s, pl.ds(b * rows, rows)]
            dst = dq_out.at[:, at((SLOTS * j + mine[j]) * n_st + s, width)]
            here = (k == kk) & (bit_of(h, j) == b)

            @pl.when(jnp.logical_not(here))
            def _():
                pltpu.make_async_remote_copy(
                    src_ref=src, dst_ref=dst,
                    send_sem=dq_send.at[j, (k + kk) % 2], recv_sem=dq_recv.at[j],
                    device_id=(2 * z + kk, h + (1 << j % 2) * (b - bit_of(h, j))), device_id_type=MESH,
                ).start()

            @pl.when(here)
            def _():
                pltpu.make_async_copy(src, dst, dq_recv.at[j]).start()

    def red_copy(j, i, n):
        mask = masks(j)[n]
        return pltpu.make_async_remote_copy(
            src_ref=red_out.at[j, i, :, at(place(flip(h, mask), j), pair)], dst_ref=red_in.at[j, i, n],
            send_sem=red_send.at[j, i], recv_sem=red_recv.at[j, i],
            device_id=(c, flip(h, mask)), device_id_type=MESH,
        )

    group = n_head // 2

    def part_copy(j, i, e):
        return pltpu.make_async_remote_copy(
            src_ref=part_out.at[j, i, :, pl.ds(e * rows, rows)],
            dst_ref=tot_in.at[j, mine[j], group + (1 if i == 0 else 0)],
            send_sem=part_send.at[j, i, e], recv_sem=tot_recv.at[j, mine[j], group + (1 if i == 0 else 0)],
            device_id=((2 * z - BACK + i + n_ctx) % n_ctx, 2 * place(h, j) + e), device_id_type=MESH,
        )

    def tot_copy(j, p):
        dk, dh = p
        return pltpu.make_async_remote_copy(
            src_ref=red_out.at[j, BACK + flip(k, dk), :, at(flip(h, dh), rows)],
            dst_ref=tot_in.at[j, mine[j], place(h, j)],
            send_sem=tot_send.at[j, dk, dh], recv_sem=tot_recv.at[j, mine[j], place(h, j)],
            device_id=dev(dk, dh), device_id_type=MESH,
        )

    def start_kv(j):
        for p in others:
            for t in range(2):
                kv_copy(j, t, p).start()

    def start_in(j, s):
        for db in range(2):
            for dk in range(2):
                for t in range(2):
                    in_copy(j, s, t, dk, db).start()

    tile = HD
    lane = lax.broadcasted_iota(jnp.int32, (8, blk), 1)

    def make_bias(j, kk):
        shift = 1 << j % 2
        block = 2 * z + kk
        docs = jnp.broadcast_to(
            doc_ref[:, pl.ds(pl.multiple_of(block * blk, blk), blk)].astype(jnp.float32), (8, blk)
        )
        first = h - shift * bit_of(h, j)
        query_doc = jnp.zeros((8, blk), jnp.float32)
        for u in range(heads):
            for b in range(2):
                to = (2 * u + b) * rows
                turn = (to - (first + b * shift) * rows + 2 * blk) % blk
                query_doc = jnp.where(lane // rows == 2 * u + b, pltpu.roll(docs, turn, 1), query_doc)
        query_doc = query_doc[:1]
        col = lax.broadcasted_iota(jnp.int32, (tile, blk), 1)
        i = (first + (col // rows) % 2 * shift) * rows + col % rows
        for part in range(4 * blk // tile):
            key_blk = jnp.maximum(block - BACK + part * tile // blk, 0)
            start = pl.multiple_of(key_blk * blk + part * tile % blk, tile)
            key_row = doc_ref[:, pl.ds(start, tile)].astype(jnp.float32)
            key_doc = jnp.transpose(jnp.broadcast_to(key_row, (tile, tile)))
            key_doc = jnp.concatenate([key_doc] * (blk // tile), axis=1)
            row = lax.broadcasted_iota(jnp.int32, (tile, blk), 0) + part * tile
            ok = (row > i) & (row <= i + BACK * blk) & (row + (block - BACK) * blk >= 0)
            ok = ok & (key_doc == query_doc)
            bias[j, kk, pl.ds(part * tile, tile)] = jnp.where(ok, 0.0, -1e30)

    def gather_and_send_up(j):
        for dh in range(n_head):
            kv_arrived(j, dh)

            @pl.when(has_up)
            def _():
                for kk in (1, 0):
                    up_copy(j, kk, dh).start()

            yield

    def fill(j):
        @pl.when(z < 1)
        def _():
            kv_buf[j, 1:3] = jnp.zeros((2,) + kv_buf.shape[2:], kv_buf.dtype)

        @pl.when(z < 2)
        def _():
            kv_buf[j, 0] = jnp.zeros(kv_buf.shape[2:], kv_buf.dtype)

    def wait_down(j):
        @pl.when(has_down)
        def _():
            for dh in range(n_head):
                await_bytes(kv_buf.at[j, 1, :, at(flip(h, dh), rows)], up_recv.at[j, 0, dh])

    def hand_on(j):
        @pl.when(has_down)
        def _():
            for dh in range(n_head):
                await_bytes(kv_buf.at[j, 2, :, at(flip(h, dh), rows)], up_recv.at[j, 1, dh])
                pl.when(has_up)(last_copy(j, dh).start)

    def wait_last(j):
        @pl.when(has_two)
        def _():
            await_bytes(kv_buf.at[j, 0], last_recv.at[j])

    def turn_keys(j, first, last):
        keys = kv_buf[j, first:last, 0].reshape((last - first) * blk, HD)
        kt_buf[j, :, first * blk : last * blk] = jnp.transpose(keys.astype(jnp.float32)).astype(jnp.bfloat16)

    lanes = [slice(a * HD, (a + 1) * HD) for a in range(heads)]
    log_scale = scale * math.log2(math.e)
    fine = 32
    tiles = 4 * blk // fine

    def stacked(j, kk, s, t):
        return jnp.concatenate([qg_buf[j, kk, s, t, :, a] for a in lanes], axis=0)

    def fold(x, op):
        return op(x.reshape(x.shape[0] // 8, 8, blk), axis=0)

    def scores(step, slot, made):
        j, kk, s = step
        q, g = stacked(j, kk, s, 0), stacked(j, kk, s, 1)
        high = None
        for n in range(4):
            s_t = lax.dot_general(kv_buf[j, kk + n, 0], q, NT, preferred_element_type=jnp.float32)
            p_t = lax.dot_general(kv_buf[j, kk + n, 1], g, NT, preferred_element_type=jnp.float32)
            for m in range(blk // fine):
                span, part = pl.ds(n * blk + m * fine, fine), slice(m * fine, (m + 1) * fine)
                one = s_t[part] + bias[j, kk, span]
                s_buf[slot][span] = one
                p_buf[slot][span] = p_t[part]
                one = fold(one, jnp.max)
                high = one if high is None else jnp.maximum(high, one)
                yield
        made["top"] = jnp.max(high, axis=0, keepdims=True)

    def exponentials(slot, made):
        top = made["top"]
        total = None
        for n in range(tiles):
            span = pl.ds(n * fine, fine)
            e_t = jnp.exp2((s_buf[slot][span] - top) * log_scale)
            s_buf[slot][span] = e_t
            one = fold(e_t, jnp.sum)
            total = one if total is None else total + one
            yield
        made["inverse"] = 1.0 / jnp.sum(total, axis=0, keepdims=True)

    def weights(slot, to, made):
        inverse = made["inverse"]
        total = None
        for n in range(tiles):
            span = pl.ds(n * fine, fine)
            w_t = s_buf[slot][span] * inverse
            s_buf[slot][span] = w_t
            w_bf = w_t.astype(jnp.bfloat16)
            w_buf[to][span] = w_bf
            one = fold(w_bf.astype(jnp.float32) * p_buf[slot][span], jnp.sum)
            total = one if total is None else total + one
            yield
        made["delta"] = jnp.sum(total, axis=0, keepdims=True)

    def differences(slot, to, made):
        delta = made["delta"]
        for n in range(tiles):
            span = pl.ds(n * fine, fine)
            d_buf[to][span] = (s_buf[slot][span] * (p_buf[slot][span] - delta)).astype(jnp.bfloat16)
            yield

    def gradients(step, slot, slot_w):
        j, kk, s = step
        q, g = stacked(j, kk, s, 0), stacked(j, kk, s, 1)
        for n in range(4):
            span = pl.ds(n * blk, blk)
            for t, left, right in ((1, w_buf[slot_w], g), (0, d_buf[slot], q)):
                more = jnp.dot(left[span], right, preferred_element_type=jnp.float32)
                for m in range(0, blk, 2 * fine):
                    acc[j, kk + n, t, pl.ds(m, 2 * fine)] += more[m : m + 2 * fine]
                    yield
        keys_t = kt_buf[j, :, kk * blk : (kk + 4) * blk]
        dq_t = jnp.dot(keys_t, d_buf[slot][...], preferred_element_type=jnp.float32)
        dq = jnp.transpose(dq_t * scale).astype(jnp.bfloat16)
        for n, a in enumerate(lanes):
            dq_buf[j, kk, s, :, a] = dq[n * pair : (n + 1) * pair]

    def in_turns(pieces):
        pieces = list(pieces)
        while pieces:
            pieces = [p for p in pieces if next(p, "end") != "end"]

    need = (has_two, has_down, has_down)

    def round_out(j, i):
        red_out[j, i, 0] = (acc[j, i, 0] * scale).astype(jnp.bfloat16)
        red_out[j, i, 1] = acc[j, i, 1].astype(jnp.bfloat16)

    def share(j, i):
        round_out(j, i)

        @pl.when(need[i])
        def _():
            for n in range(len(masks(j))):
                red_copy(j, i, n).start()

    def send_part(j, i):
        @pl.when(need[i])
        def _():
            await_bytes(red_in.at[j, i], red_recv.at[j, i])
            mine_here = at(place(h, j), pair)
            sums = [acc[j, i, 0, mine_here] * scale, acc[j, i, 1, mine_here]]
            for t in range(2):
                for n in range(len(masks(j))):
                    sums[t] = sums[t] + red_in[j, i, n, t].astype(jnp.float32)
                part_out[j, i, t] = sums[t].astype(jnp.bfloat16)
            for e in range(2):
                part_copy(j, i, e).start()

    def send_own(j):
        for kk in range(2):
            round_out(j, BACK + kk)
        for p in others:
            tot_copy(j, p).start()
        tot_in[j, mine[j], place(h, j)] = red_out[j, BACK + k, :, at(h, rows)]

    for j in range(jobs):
        fill(j)
        acc[j] = jnp.zeros(acc.shape[1:], acc.dtype)
        for kk in range(2):
            make_bias(j, kk)

    pl.semaphore_wait(barrier, len(others) + 2 + 6 * jobs)
    for t in range(2):
        await_bytes(own_buf.at[t], own_sem.at[t])
    start_kv(0)
    start_in(0, 0)
    start_in(0, 1)
    for j in range(1, jobs):
        start_kv(j)
    for j in range(jobs):
        @pl.loop(2 if j == 0 else 0, n_st)
        def _(s):
            start_in(j, s)

    for _ in gather_and_send_up(0):
        pass
    hand_on(0)
    wait_down(0)
    turn_keys(0, 1, 5)

    steps = []
    half = n_st // 2
    for j in range(jobs):
        if j == 0:
            order = [(kk, s) for kk in (1, 0) for s in range(half)] + [(kk, s) for s in range(half, n_st) for kk in (1, 0)]
        else:
            order = [(1, s) for s in range(half)] + [(0, s) for s in range(n_st)] + [(1, s) for s in range(half, n_st)]
        steps += [(j, kk, s) for kk, s in order]
    per_job = 2 * n_st

    def before(n):
        j, first = n // per_job, n % per_job
        if j > 0 and first == 0:
            wait_down(j)
            turn_keys(j, 1, 5)
        if first == half:
            wait_last(j)
            turn_keys(j, 0, 1)
        if first == 1 and j + 1 < jobs:
            for _ in gather_and_send_up(j + 1):
                pass
        if first == per_job - 2 and j + 1 < jobs:
            hand_on(j + 1)
        in_arrived(*steps[n][:1], steps[n][2], steps[n][1])

    def after(n):
        j, first = n // per_job, n % per_job
        dq_send_out(j, steps[n][2], steps[n][1])
        last = j == jobs - 1
        if j > 0 and first == per_job // 2:
            send_part(j - 1, 0)
            send_part(j - 1, 1)
        if j > 0 and first == half + n_st - 1:
            share(j, 0)
        if first == per_job - 1:
            for i in range(1 if j > 0 else 0, BACK):
                share(j, i)
            send_own(j)
            if j > 0:
                send_part(j - 1, 2)
            if last:
                for i in range(BACK):
                    send_part(j, i)

    made = [{} for _ in steps]
    for n in range(len(steps) + 4):
        pieces = []
        if n < len(steps):
            before(n)
        if 0 <= n - 4:
            pieces.append(gradients(steps[n - 4], n % 2, (n - 4) % 3))
        if n < len(steps):
            pieces.append(scores(steps[n], n % 4, made[n]))
        if 0 <= n - 1 < len(steps):
            pieces.append(exponentials((n - 1) % 4, made[n - 1]))
        if 0 <= n - 2 < len(steps):
            pieces.append(weights((n - 2) % 4, (n - 2) % 3, made[n - 2]))
        if 0 <= n - 3 < len(steps):
            pieces.append(differences((n - 3) % 4, (n - 3) % 2, made[n - 3]))
        in_turns(pieces)
        if 0 <= n - 4:
            after(n - 4)

    for j in range(jobs):
        for slot in range(SLOTS):
            n = SLOTS * j + slot
            for o in range(group):
                @pl.when((mine[j] != slot) | (place(h, j) != o))
                def _():
                    await_bytes(tot_in.at[j, slot, o], tot_recv.at[j, slot, o])

            for far, cond in ((0, has_up), (1, (z + 2 < n_z) & (k == 1))):
                @pl.when(cond)
                def _():
                    await_bytes(tot_in.at[j, slot, group + far], tot_recv.at[j, slot, group + far])

                @pl.when(jnp.logical_not(cond))
                def _():
                    tot_in[j, slot, group + far] = jnp.zeros(tot_in.shape[3:], tot_in.dtype)

            for t in range(2):
                total = tot_in[j, slot, 0, t].astype(jnp.float32)
                for o in range(1, group + 2):
                    total = total + tot_in[j, slot, o, t].astype(jnp.float32)
                (dk_out, dv_out)[t][:, n * HD : (n + 1) * HD] = total

    for j in range(jobs):
        await_bytes(dq_buf.at[j, 0], in_send.at[j, 0])
        await_bytes(qg_buf.at[j, 0], in_send.at[j, 1])
        await_bytes(dq_buf.at[j, 0, :, pl.ds(0, rows)], dq_send.at[j, 0])
        await_bytes(dq_buf.at[j, 0], dq_send.at[j, 1])
        await_bytes(qg_buf.at[j, 0], dq_recv.at[j])
        await_bytes(kv_buf.at[j, 0, :, pl.ds(0, rows)], kv_send.at[j, 0])
        for dh in range(1, n_head):
            await_bytes(kv_buf.at[j, 0:2, :, pl.ds(0, rows)], kv_send.at[j, dh])
        for p in others:
            tot_copy(j, p).wait_send()

        for i in range(BACK):
            @pl.when(need[i])
            def _():
                await_bytes(red_in.at[j, i], red_send.at[j, i])
                for e in range(2):
                    part_copy(j, i, e).wait_send()

        @pl.when(has_up)
        def _():
            await_bytes(kv_buf.at[j, 0:2], up_send.at[j])

        @pl.when(has_up & has_down)
        def _():
            await_bytes(kv_buf.at[j, 0], last_send.at[j])


def widen(*refs):
    src, dst, near, wide, (get, put) = refs[:3], refs[3:6], refs[6:9], refs[9:12], refs[12:]
    step = src[0].shape[1] // CUTS
    pieces = [(0, pl.ds(n * step, step)) for n in range(CUTS)] + [(n, pl.ds(0, src[n].shape[1])) for n in (1, 2)]
    reads = [pltpu.make_async_copy(src[a].at[:, s], near[a].at[:, s], get.at[n]) for n, (a, s) in enumerate(pieces)]
    writes = [pltpu.make_async_copy(wide[a].at[:, s], dst[a].at[:, s], put.at[n]) for n, (a, s) in enumerate(pieces)]
    for read in reads:
        read.start()
    for (a, s), read, write in zip(pieces, reads, writes):
        read.wait()
        wide[a][:, s] = near[a][:, s].astype(jnp.float32)
        write.start()
    for write in writes:
        write.wait()


def body(queries, keys, values, out_grad, doc_ids):
    n_ctx, n_head = lax.axis_size("ctx"), lax.axis_size("head")
    rows, q_cols = queries.shape
    kv_cols = keys.shape[1]
    blk = rows * n_head
    jobs = kv_cols // HD // SLOTS
    group = q_cols // kv_cols
    heads = n_head // 2
    n_st = group // heads
    pair = 2 * rows
    win = BACK + 2
    bf, f32, dma = jnp.bfloat16, jnp.float32, pltpu.SemaphoreType.DMA
    far = pl.BlockSpec(memory_space=pl.ANY)
    near = pl.BlockSpec(memory_space=pltpu.VMEM)
    dq, dk, dv = pl.pallas_call(
        functools.partial(kernel, n_ctx, n_head),
        out_shape=(
            jax.ShapeDtypeStruct((rows, q_cols), bf),
            jax.ShapeDtypeStruct((rows, kv_cols), f32),
            jax.ShapeDtypeStruct((rows, kv_cols), f32),
        ),
        in_specs=[far, far, far, far, near],
        out_specs=(far, near, near),
        scratch_shapes=[
            pltpu.VMEM((2, rows, kv_cols), bf),
            pltpu.VMEM((jobs, 2, n_st, 2, pair, heads * HD), bf),
            pltpu.VMEM((jobs, 2, n_st, pair, heads * HD), bf),
            pltpu.VMEM((jobs, win, 2, blk, HD), bf),
            pltpu.VMEM((jobs, HD, win * blk), bf),
            pltpu.VMEM((jobs, win, 2, blk, HD), f32),
            pltpu.VMEM((jobs, 2, 4 * blk, blk), f32),
            pltpu.VMEM((jobs, win, 2, blk, HD), bf),
            pltpu.VMEM((jobs, BACK, n_head // 2 - 1, 2, pair, HD), bf),
            pltpu.VMEM((jobs, BACK, 2, pair, HD), bf),
            pltpu.VMEM((jobs, SLOTS, n_head // 2 + 2, 2, rows, HD), bf),
            (pltpu.VMEM((4 * blk, blk), f32),) * 4,
            (pltpu.VMEM((4 * blk, blk), f32),) * 4,
            (pltpu.VMEM((4 * blk, blk), bf),) * 3,
            (pltpu.VMEM((4 * blk, blk), bf),) * 2,
            dma((2,)),
            dma((jobs, n_head)),
            dma((jobs, n_head)),
            dma((jobs, 2)),
            dma((jobs, n_st, 2)),
            dma((jobs,)),
            dma((jobs, 2, n_head)),
            dma((jobs,)),
            dma((jobs,)),
            dma((jobs, 2)),
            dma((jobs,)),
            dma((jobs, BACK)),
            dma((jobs, BACK)),
            dma((jobs, BACK, 2)),
            dma((jobs, 2, n_head)),
            dma((jobs, SLOTS, n_head // 2 + 2)),
        ],
        compiler_params=pltpu.CompilerParams(
            collective_id=0, has_side_effects=True, vmem_limit_bytes=56 * 2**20,
        ),
    )(queries, keys, values, out_grad, doc_ids.reshape(1, -1))
    outs = [jax.ShapeDtypeStruct(x.shape, f32) for x in (dq, dk, dv)]
    return pl.pallas_call(
        widen,
        out_shape=outs,
        in_specs=[far] * 3,
        out_specs=[far] * 3,
        scratch_shapes=[
            *[pltpu.VMEM(x.shape, x.dtype) for x in (dq, dk, dv)],
            *[pltpu.VMEM(x.shape, f32) for x in (dq, dk, dv)],
            dma((CUTS + 2,)),
            dma((CUTS + 2,)),
        ],
    )(dq, dk, dv)


def solution(mesh):
    split = P(("ctx", "head"), None)
    return jax.shard_map(
        body,
        mesh=mesh,
        in_specs=(split, split, split, split, P()),
        out_specs=(split, split, split),
        check_vma=False,
    )
```
